32 devices in a mesh: ctx: 8 (over y, x, core), tensor: 4 (over z).
Axes of the slice: x: 2, y: 2, z: 4, core: 2. Of those that a mesh axis runs over, the one named last changes fastest.
Arguments:
- queries: bfloat16 [8192, 4096], P('ctx', 'tensor'), may hold values from -6 to 6
- keys: bfloat16 [8192, 4096], P('ctx', 'tensor'), may hold values from -6 to 6
- values: bfloat16 [8192, 4096], P('ctx', 'tensor'), may hold values from -6 to 6
- doc_ids: int32 [8192], P('ctx'), may hold values from 0 to 7, never falling along the last dimension, each value on 1 to 4096 neighbouring positions
- out_weight: bfloat16 [4096, 6144], P('tensor'), may hold values from -0.125 to 0.125
- grad_out: bfloat16 [8192, 6144], P('ctx', 'tensor'), may hold values from -6 to 6
Outputs:
- attended: bfloat16 [8192, 6144], P('ctx', 'tensor')
- grad_queries: bfloat16 [8192, 4096], P('ctx', 'tensor')
- grad_keys: bfloat16 [8192, 4096], P('ctx', 'tensor')
- grad_values: bfloat16 [8192, 4096], P('ctx', 'tensor')
- grad_weight: float32 [4096, 6144], P('tensor', 'ctx')
The draws below stay inside these ranges and needn't reach their ends.
Inputs may be any that keep to these rules, and one draw needn't show every extreme that they name: `doc_ids`: never falling along the sequence; each document has 1 to 4096 positions, and one has exactly 4096.
All inputs are finite; a program needn't handle non-finite values.
Results may differ from the reference program's by a relative error of at most 0.015.
Values may be sent and summed in bfloat16 or wider, within the bound.
A program may use at most 192 MiB of HBM per device.

```python
import math
import jax
import jax.numpy as jnp
import numpy as np
from jax import lax

D = 6144
HEADS = 32
HEAD = 128
DOCS = 8
TOK_DEV = 1024
LENGTH = 8192
N_TENSOR = 4


def with_spikes(values, rng, source, target, shards_of, factor):
    def block_of(dim):
        return (jnp.arange(values.shape[dim]) // (values.shape[dim] // shards_of)).reshape((-1,) + (1,) * (values.ndim - 1 - dim))

    one_side = jax.random.permutation(rng, shards_of)[block_of(target)]
    second = (block_of(target) + shards_of // 2) % shards_of
    return jnp.where((block_of(source) == one_side) | (block_of(source) == second), factor * values, values)


def block_scale(key, extent, shards, smallest, high):
    loudness = 1.0
    for axis_at, blocks in shards:
        heights = jax.random.uniform(jax.random.fold_in(jax.random.fold_in(key, 6), axis_at), (blocks,), jnp.float32, smallest / len(shards), high / len(shards))
        loudness = loudness * jnp.repeat(jnp.exp(heights), extent[axis_at] // blocks).reshape((-1,) + (1,) * (len(extent) - 1 - axis_at))
    return loudness


def length_profile(amount, total, bound, skew):
    loads = [(1 << 20) // math.isqrt(grade ** skew) + 1 for grade in range(2, amount + 1)]
    rest, given = total - bound - (amount - 1), [1] * (amount - 1)
    while rest > 0:
        free = [i for i in range(amount - 1) if given[i] < bound]
        mass, remaining = sum([loads[i] for i in free]), rest
        for i in free:
            more = min(bound - given[i], max(1, remaining * loads[i] // mass), rest)
            given[i] = given[i] + more
            rest = rest - more
    return np.array([bound] + given)


def uneven(stream_key, number_of, total, limit, skew):
    if number_of == 2:
        one = jax.random.randint(stream_key, (), max(1, total - limit), min(limit, total - 1) + 1)
        return jnp.stack([one, total - one])
    tallies = jnp.asarray(length_profile(number_of, total, limit, skew), jnp.int32)
    pairs = (number_of - 1) // 2
    source_of, sink = tallies[1:1 + 2 * pairs:2], tallies[2:2 + 2 * pairs:2]
    room = jnp.minimum(source_of - 1, limit - sink)
    moved = jax.random.randint(jax.random.fold_in(stream_key, 1), (pairs,), 0, 1 << 20) % (room + 1)
    tallies = tallies.at[1:1 + 2 * pairs:2].set(source_of - moved).at[2:2 + 2 * pairs:2].set(sink + moved)
    return tallies[jax.random.permutation(jax.random.fold_in(stream_key, 2), number_of)]


def scatter_about(rng, shape, spread, limit, pieces=(), dtype=jnp.bfloat16):
    entries = spread * jax.random.normal(rng, shape, jnp.float32)
    if pieces:
        entries = entries * block_scale(rng, shape, pieces, -0.22, 0.18)
    return jnp.clip(entries, -limit, limit).astype(dtype)


def gaussian_with(rng, shape, spread, reach, cuts, heavy, dtype=jnp.bfloat16):
    values = spread * jax.random.normal(rng, shape, jnp.float32)
    if cuts:
        values = values * block_scale(rng, shape, cuts, -0.22, 0.18)
    return jnp.clip(with_spikes(values, jax.random.fold_in(rng, 3), *heavy), -reach, reach).astype(dtype)


def setup_inputs(seed: int = 0) -> dict:
    streams_of = jax.random.split(jax.random.key(seed), 7)
    queries = scatter_about(streams_of[0], (LENGTH, HEADS * HEAD), 1.0, 6.0, ((0, 8), (1, 4)))
    keys = scatter_about(streams_of[1], (LENGTH, HEADS * HEAD), 1.0, 6.0, ((0, 8), (1, 4)))
    values = scatter_about(streams_of[2], (LENGTH, HEADS * HEAD), 1.0, 6.0, ((0, 8), (1, 4)))
    doc_ids = jnp.searchsorted(jnp.cumsum(uneven(streams_of[3], DOCS, LENGTH, LENGTH // 2, 1)), jnp.arange(LENGTH), side="right").astype(jnp.int32)
    out_weight = gaussian_with(streams_of[4], (HEADS * HEAD, D), (HEADS * HEAD) ** -0.5, 0.125, ((0, 4),), (0, 1, 4, 2.0))
    grad_out = gaussian_with(streams_of[5], (LENGTH, D), 1.0, 6.0, ((0, 8), (1, 4)), (0, 1, 8, 2.0))
    return {"queries": queries, "keys": keys, "values": values, "doc_ids": doc_ids, "out_weight": out_weight, "grad_out": grad_out}


highest = lax.Precision.HIGHEST
epsilon = 1e-06

def attend(query_float, key_float, value_float, doc_ids):
    blocks = LENGTH // TOK_DEV
    order = jnp.arange(TOK_DEV)
    causal = order[:, None] >= order[None, :]

    def shaped(array):
        return array.reshape(blocks, TOK_DEV, HEADS, HEAD)

    def advance(carry, block):
        state, last_doc = carry
        query, key, value, documents = block
        mask = (causal & (documents[:, None] == documents[None, :])).astype(jnp.float32)
        scores = jnp.einsum('the,uhe->htu', query, key, precision=highest) * mask[None]
        local = jnp.einsum('htu,uhf->thf', scores, value, precision=highest)
        carried = jnp.einsum('the,hef->thf', query, state, precision=highest)
        joined = (documents == last_doc).astype(jnp.float32)[:, None, None]
        output = local + joined * carried
        tail = (documents == documents[-1]).astype(jnp.float32)[:, None, None]
        added = jnp.einsum('uhe,uhf->hef', key * tail, value, precision=highest)
        keeping = (documents[-1] == last_doc).astype(jnp.float32)
        return ((added + keeping * state, documents[-1]), output)
    start = (jnp.zeros((HEADS, HEAD, HEAD), jnp.float32), jnp.array(-1, jnp.int32))
    final_carry, outputs = lax.scan(advance, start, (shaped(query_float), shaped(key_float), shaped(value_float), doc_ids.reshape(blocks, TOK_DEV).astype(jnp.int32)))
    return outputs.reshape(LENGTH, HEADS, HEAD)

def reference(queries, keys, values, doc_ids, out_weight, grad_out):
    query_float = queries.astype(jnp.float32).reshape(LENGTH, HEADS, HEAD)
    key_float = keys.astype(jnp.float32).reshape(LENGTH, HEADS, HEAD)
    value_float = values.astype(jnp.float32).reshape(LENGTH, HEADS, HEAD)

    def forward(query_in, key_in, value_in):
        return attend(query_in, key_in, value_in, doc_ids)
    opened, pullback = jax.vjp(forward, query_float, key_float, value_float)
    inverse = lax.rsqrt(lax.optimization_barrier(jnp.mean(opened * opened, axis=-1, keepdims=True)) + epsilon)
    normed = opened * inverse
    normed_low = normed.reshape(LENGTH, HEADS * HEAD).astype(jnp.bfloat16)
    group = HEADS * HEAD // N_TENSOR
    total = jnp.zeros((LENGTH, D), jnp.float32)
    for index in range(N_TENSOR):
        part = jnp.dot(normed_low[:, index * group:(index + 1) * group], out_weight[index * group:(index + 1) * group], preferred_element_type=jnp.float32)
        total = total + part.astype(jnp.bfloat16).astype(jnp.float32)
    attended = total.astype(jnp.bfloat16)
    grad_normed = lax.dot_general(grad_out, out_weight, (((1,), (1,)), ((), ())), preferred_element_type=jnp.float32)
    grad_weight = lax.dot_general(normed_low, grad_out, (((0,), (0,)), ((), ())), preferred_element_type=jnp.float32)
    grad_normed = grad_normed.reshape(LENGTH, HEADS, HEAD)
    grad_opened = inverse * (grad_normed - normed * lax.optimization_barrier(jnp.mean(grad_normed * normed, axis=-1, keepdims=True)))
    grad_query, grad_key, grad_value = pullback(grad_opened)
    width = HEADS * HEAD
    return (attended, grad_query.reshape(LENGTH, width).astype(jnp.bfloat16), grad_key.reshape(LENGTH, width).astype(jnp.bfloat16), grad_value.reshape(LENGTH, width).astype(jnp.bfloat16), grad_weight)
```

```python
import functools

import jax
import jax.numpy as jnp
from jax import lax
from jax.experimental import pallas as pl
from jax.experimental.pallas import tpu as pltpu
from jax.sharding import PartitionSpec as P

HEAD = 128
CHUNK = 256
epsilon = 1e-06
f32 = jnp.float32
bf16 = jnp.bfloat16


def dot(a, b, ca, cb):
    return lax.dot_general(a, b, (((ca,), (cb,)), ((), ())), preferred_element_type=f32)


def params():
    return pltpu.CompilerParams(
        dimension_semantics=("arbitrary",), vmem_limit_bytes=48 * 1024 * 1024
    )


def cost(flops, moved):
    return pl.CostEstimate(flops=int(flops), bytes_accessed=int(moved), transcendentals=0)


def masked(values, col, row, start, stop):
    rows, cols = values.shape
    r = lax.broadcasted_iota(jnp.int32, (rows, cols), 0) + start
    c = lax.broadcasted_iota(jnp.int32, (rows, cols), 1)
    keep = (r >= c) & (col[start:stop, :] == row[:, :cols])
    return jnp.where(keep, values, 0.0).astype(bf16)


def tail_kernel(heads, k_ref, v_ref, col_ref, out_ref):
    h = pl.program_id(0)
    rows = k_ref.shape[0]
    last = col_ref[rows - 1 : rows, :]

    @pl.when(h < heads)
    def _():
        mask = (col_ref[...] == last).astype(f32)
        km = (k_ref[...].astype(f32) * mask).astype(bf16)
        out_ref[...] = dot(km, v_ref[...], 0, 0).astype(bf16)

    @pl.when(h == heads)
    def _():
        r = lax.broadcasted_iota(jnp.int32, out_ref.shape, 0)
        first = col_ref[0:1, :]
        out_ref[...] = jnp.where(r < HEAD // 2, last, first).astype(bf16)


def local_kernel(q_ref, k_ref, v_ref, col_ref, row_ref, out_ref):
    rows = q_ref.shape[0]
    for start in range(0, rows, CHUNK):
        stop = start + CHUNK
        s = dot(q_ref[start:stop, :], k_ref[:stop, :], 1, 1)
        s = masked(s, col_ref, row_ref, start, stop)
        out_ref[start:stop, :] = dot(s, v_ref[:stop, :], 1, 0)


def norm_kernel(local_ref, q_ref, state_ref, joined_ref, opened_ref, low_ref):
    opened = local_ref[...] + joined_ref[...] * dot(q_ref[...], state_ref[...], 1, 0)
    inverse = lax.rsqrt(jnp.mean(opened * opened, axis=-1, keepdims=True) + epsilon)
    opened_ref[...] = opened
    low_ref[...] = (opened * inverse).astype(bf16)


def open_kernel(gn_ref, opened_ref, q_ref, head_ref, g_ref, state_ref):
    opened = opened_ref[...]
    gn = gn_ref[...]
    inverse = lax.rsqrt(jnp.mean(opened * opened, axis=-1, keepdims=True) + epsilon)
    normed = opened * inverse
    g = inverse * (gn - normed * jnp.mean(gn * normed, axis=-1, keepdims=True))
    g = g.astype(bf16)
    g_ref[...] = g
    qm = (q_ref[...].astype(f32) * head_ref[...]).astype(bf16)
    state_ref[...] = dot(qm, g, 0, 0).astype(bf16)


def back_kernel(
    q_ref, k_ref, v_ref, g_ref, col_ref, row_ref, joined_ref, state_ref, dq_ref, dk_ref, dv_ref
):
    rows = q_ref.shape[0]
    for start in reversed(range(0, rows, CHUNK)):
        stop = start + CHUNK
        q, g = q_ref[start:stop, :], g_ref[start:stop, :]
        s = masked(dot(q, k_ref[:stop, :], 1, 1), col_ref, row_ref, start, stop)
        ds = masked(dot(g, v_ref[:stop, :], 1, 1), col_ref, row_ref, start, stop)
        dq = dot(ds, k_ref[:stop, :], 1, 0)
        dq = dq + joined_ref[start:stop, :] * dot(g, state_ref[...], 1, 1)
        dq_ref[start:stop, :] = dq.astype(bf16)
        dk, dv = dot(ds, q, 0, 0), dot(s, g, 0, 0)
        if stop == rows:
            dk_ref[...] = dk
            dv_ref[...] = dv
        else:
            dk_ref[:stop, :] += dk
            dv_ref[:stop, :] += dv


def final_kernel(dk_ref, dv_ref, k_ref, v_ref, starts_ref, state_ref, dko_ref, dvo_ref):
    starts = starts_ref[...]
    state = state_ref[...]
    dko_ref[...] = (dk_ref[...] + starts * dot(v_ref[...], state, 1, 1)).astype(bf16)
    dvo_ref[...] = (dv_ref[...] + starts * dot(k_ref[...], state, 1, 0)).astype(bf16)


def body(n, n_ctx, queries, keys, values, doc_ids, out_weight, grad_out):
    rows, width = queries.shape
    heads = width // HEAD
    part = grad_out.shape[1]
    half = part // 2
    me = lax.axis_index("tensor")
    place = lax.axis_index("ctx")
    doc = doc_ids.astype(f32)
    col, row = doc[:, None], doc[None, :]

    wide = pl.BlockSpec((rows, HEAD), lambda h: (0, h))
    square = pl.BlockSpec((HEAD, HEAD), lambda h: (h, 0))
    colspec = pl.BlockSpec((rows, 1), lambda h: (0, 0))
    rowspec = pl.BlockSpec((1, rows), lambda h: (0, 0))
    shape = jax.ShapeDtypeStruct
    unit = 2 * rows * rows * width
    small = 2 * rows * HEAD * width

    def tied(moved, done):
        return lax.optimization_barrier((*moved, *done))[: len(moved)]

    def gather(block, ties):
        right = left = block
        got = {0: block}
        for s in range(1, n):
            right, left = tied((right, left), ties.get(s, ()))
            right = lax.ppermute(right, "tensor", [(i, i + 1) for i in range(s - 1, n - 1)])
            left = lax.ppermute(left, "tensor", [(i, i - 1) for i in range(1, n - s + 1)])
            got[s], got[-s] = right, left
        blocks = []
        for b in range(n):
            value = None
            for i in range(n):
                piece = got[i - b]
                value = piece if value is None else jnp.where(me == i, piece, value)
            blocks.append(value)
        return jnp.concatenate(blocks, axis=1)

    clipped = pl.BlockSpec((rows, HEAD), lambda h: (0, jnp.minimum(h, heads - 1)))
    tail = pl.pallas_call(
        functools.partial(tail_kernel, heads),
        grid=(heads + 1,),
        in_specs=[clipped, clipped, colspec],
        out_specs=square,
        out_shape=shape(((heads + 1) * HEAD, HEAD), bf16),
        compiler_params=params(),
        cost_estimate=cost(small, 4 * rows * width),
        name="tail",
    )(keys, values, col)
    tails = lax.all_gather(tail, "ctx")
    local = pl.pallas_call(
        local_kernel,
        grid=(heads,),
        in_specs=[wide, wide, wide, colspec, rowspec],
        out_specs=wide,
        out_shape=shape((rows, width), f32),
        compiler_params=params(),
        cost_estimate=cost(2 * unit, 10 * rows * width),
        name="local",
    )(queries, keys, values, col, row)
    wholes = [gather(grad_out[:, :half], {2: (tail,), 3: (local,)})]
    last_docs = tails[:, heads * HEAD, 0].astype(f32)
    first_docs = tails[:, heads * HEAD + HEAD // 2, 0].astype(f32)
    index = jnp.arange(n_ctx)
    last_doc = jnp.sum(jnp.where(index == place - 1, last_docs, 0.0)) - (place == 0)
    first_doc = jnp.sum(jnp.where(index == place + 1, first_docs, 0.0)) - (place == n_ctx - 1)
    before = (index < place) & (last_docs == last_doc)
    after = (index > place) & (first_docs == first_doc)
    joined = (col == last_doc).astype(f32)
    starts = (col == first_doc).astype(f32)

    def total(parts, reached):
        picked = jnp.where(reached[:, None, None], parts.astype(f32), 0.0)
        return jnp.sum(picked, axis=0).astype(bf16)

    state_in = total(tails[:, : heads * HEAD], before)
    opened, normed_low = pl.pallas_call(
        norm_kernel,
        grid=(heads,),
        in_specs=[wide, wide, square, colspec],
        out_specs=[wide, wide],
        out_shape=[shape((rows, width), f32), shape((rows, width), bf16)],
        compiler_params=params(),
        cost_estimate=cost(small, 12 * rows * width),
        name="norm",
    )(local, queries, state_in, joined)

    partial_out = dot(normed_low, out_weight, 1, 0).astype(bf16)

    def term(d):
        d = jnp.clip(d, 0, n - 1)
        return lax.dynamic_slice_in_dim(partial_out, d * part, part, axis=1)

    def products(j, whole):
        weight = jnp.concatenate(
            [out_weight[:, b * part + j * half : b * part + (j + 1) * half] for b in range(n)], axis=1
        )
        weight_term = dot(normed_low, whole, 0, 0).astype(bf16)
        return dot(whole, weight, 1, 1), weight_term

    def scattered(weight_term):
        return lax.psum_scatter(weight_term, "ctx", scatter_dimension=1, tiled=True)

    first = products(0, wholes[0])
    operands = {}
    def hop(s, right, left, done):
        a, b = term(me + n - s), term(me - n + s)
        if s > 1:
            a = (a.astype(f32) + right.astype(f32)).astype(bf16)
            b = (b.astype(f32) + left.astype(f32)).astype(bf16)
        operands[s] = a, b = tied((a, b), done)
        right = lax.ppermute(a, "tensor", [(i, i + 1) for i in range(s)])
        left = lax.ppermute(b, "tensor", [(i, i - 1) for i in range(n - s, n)])
        return right, left

    right = left = None
    for s in range(1, n - 1):
        right, left = hop(s, right, left, first if s == 2 else ())

    ties = {1: (normed_low,), 2: operands[1], 3: operands.get(2, ())}
    wholes.append(gather(grad_out[:, half:], ties))
    second = products(1, wholes[1])
    grad_normed = first[0] + second[0]
    pieces = [scattered(first[1]), scattered(second[1])]
    (grad_normed,) = tied((grad_normed,), (pieces[0],))

    odd = place % 2 == 1
    kept = jnp.where(odd, pieces[1], pieces[0])
    given = jnp.where(odd, pieces[0], pieces[1])
    taken = lax.ppermute(given, "ctx", [(i, i ^ 1) for i in range(n_ctx)])
    grad_weight = jnp.concatenate(
        [jnp.where(odd, taken, kept), jnp.where(odd, kept, taken)], axis=1
    ).astype(f32)

    head = (col == doc[0]).astype(f32)
    grad_opened, head_state = pl.pallas_call(
        open_kernel,
        grid=(heads,),
        in_specs=[wide, wide, wide, colspec],
        out_specs=[wide, square],
        out_shape=[shape((rows, width), bf16), shape((heads * HEAD, HEAD), bf16)],
        compiler_params=params(),
        cost_estimate=cost(small, 12 * rows * width),
        name="open",
    )(grad_normed, opened, queries, head)
    heads_all = lax.all_gather(head_state, "ctx")
    right, left = hop(n - 1, right, left, (head_state,))
    grad_query, dk, dv = pl.pallas_call(
        back_kernel,
        grid=(heads,),
        in_specs=[wide, wide, wide, wide, colspec, rowspec, colspec, square],
        out_specs=[wide, wide, wide],
        out_shape=[
            shape((rows, width), bf16),
            shape((rows, width), f32),
            shape((rows, width), f32),
        ],
        compiler_params=params(),
        cost_estimate=cost(5 * unit, 18 * rows * width),
        name="back",
    )(queries, keys, values, grad_opened, col, row, joined, state_in)
    state_back = total(heads_all, after)
    grad_key, grad_value = pl.pallas_call(
        final_kernel,
        grid=(heads,),
        in_specs=[wide, wide, wide, wide, colspec, square],
        out_specs=[wide, wide],
        out_shape=[shape((rows, width), bf16)] * 2,
        compiler_params=params(),
        cost_estimate=cost(2 * small, 16 * rows * width),
        name="final",
    )(dk, dv, keys, values, starts, state_back)
    right, left = tied((right, left), (grad_query,))
    attended = (term(me).astype(f32) + right.astype(f32) + left.astype(f32)).astype(bf16)
    return attended, grad_query, grad_key, grad_value, grad_weight


def solution(mesh):
    n, n_ctx = mesh.shape["tensor"], mesh.shape["ctx"]
    assert n_ctx == 2 * n
    return jax.shard_map(
        functools.partial(body, n, n_ctx),
        mesh=mesh,
        in_specs=(
            P("ctx", "tensor"),
            P("ctx", "tensor"),
            P("ctx", "tensor"),
            P("ctx"),
            P("tensor", None),
            P("ctx", "tensor"),
        ),
        out_specs=(
            P("ctx", "tensor"),
            P("ctx", "tensor"),
            P("ctx", "tensor"),
            P("ctx", "tensor"),
            P("tensor", "ctx"),
        ),
        check_vma=False,
    )
```
